32 devices in a mesh: dp: 4 (over z), expert: 2 (over x), shard: 4 (over y, core).
Axes of the slice: x: 2, y: 2, z: 4, core: 2. Of those that a mesh axis runs over, the one named last changes fastest.
Arguments:
- activations: bfloat16 [2, 2, 2048, 256], P(None, 'expert', ('dp', 'shard')), may hold values from -6 to 6
- out_grads: bfloat16 [2, 2, 2048, 14336], P(None, 'expert', ('dp', 'shard')), may hold values from -0.25 to 0.25
- weights: float32 [2, 2, 256, 14336], P(None, 'expert', ('dp', 'shard')), may hold values from -4 to 4
- shadow: float32 [2, 2, 256, 14336], P(None, 'expert', ('dp', 'shard')), may hold values from -4 to 4
- counts: int32 [2, 32, 2], P(None, ('dp', 'expert', 'shard')), may hold values from 1 to 1024, as said below
Outputs:
- new_weights: float32 [2, 2, 256, 14336], P(None, 'expert', ('dp', 'shard'))
- new_shadow: float32 [2, 2, 256, 14336], P(None, 'expert', ('dp', 'shard'))
The draws below stay inside these ranges and needn't reach their ends.
Inputs may be any that keep to these rules, and one draw needn't show every extreme that they name: `counts`: loads differ between the experts of a layer.
All inputs are finite; a program needn't handle non-finite values.
Results may differ from the reference program's by a relative error of at most 0.0003.
Values sent between devices are 32-bit elements; how exact they have to be, the bound alone decides.
No kernel may reach another device: no remote copies, remote signals or barrier semaphores. Data moves between devices by JAX's collectives and lax.ppermute only.
A program may use at most 128 MiB of HBM per device.

```python
import jax
import jax.numpy as jnp
from jax import lax

FF = 14336
ROWS = 256
TOK_DEV = 128
LAYERS = 2
EXPERTS = 2
TOKENS = 2048
DEVICES = 32


def draw_activations(key, part):
    base = jax.random.normal(key, (LAYERS, EXPERTS, TOKENS, ROWS), jnp.float32)
    return jnp.clip(base, -6.0, 6.0).astype(jnp.bfloat16)


def draw_out_grads(key, part):
    base = 0.03 * jax.random.normal(key, (LAYERS, EXPERTS, TOKENS, FF), jnp.float32)
    return jnp.clip(base, -0.25, 0.25).astype(jnp.bfloat16)


def draw_counts(key, part):
    ranges = jax.random.randint(jax.random.fold_in(key, 3), (LAYERS, 1, EXPERTS), 1, 9)
    raw = jax.random.randint(key, (LAYERS, DEVICES, EXPERTS), 0, 1 << 20)
    values = 1 + raw % (TOK_DEV * ranges)
    chosen_device = jax.random.randint(jax.random.fold_in(key, 5), (LAYERS, 1, 1), 0, DEVICES)
    chosen_expert = jax.random.randint(jax.random.fold_in(key, 6), (LAYERS, 1, 1), 0, EXPERTS)
    device_ids = jnp.arange(DEVICES, dtype=jnp.int32)[None, :, None]
    expert_ids = jnp.arange(EXPERTS, dtype=jnp.int32)[None, None, :]
    marked = (device_ids == chosen_device) & (expert_ids == chosen_expert)
    values = jnp.where(marked, 8 * TOK_DEV, values)
    return values.astype(jnp.int32)


def levels(key, dims, pieces, low, largest):
    level, own = 1.0, jax.random.fold_in(key, 6)
    for axis_at, parts in pieces:
        steps = jnp.exp(jax.random.uniform(jax.random.fold_in(own, axis_at), (parts,), jnp.float32, low / len(pieces), largest / len(pieces)))
        level = level * jnp.repeat(steps, dims[axis_at] // parts).reshape([-1 if axis == axis_at else 1 for axis in range(len(dims))])
    return level


def normal_values(stream_key, dims, spread, reach, pieces=(), held_as=jnp.bfloat16):
    drawn = spread * jax.random.normal(stream_key, dims, jnp.float32)
    if pieces:
        drawn = drawn * levels(stream_key, dims, pieces, -0.22, 0.18)
    return jnp.clip(drawn, -reach, reach).astype(held_as)


def setup_inputs(seed: int = 0) -> dict:
    streams_of = jax.random.split(jax.random.key(seed), 6)
    return {
        "activations": draw_activations(jax.random.fold_in(streams_of[5], 71), 0),
        "out_grads": draw_out_grads(jax.random.fold_in(streams_of[5], 71), 0),
        "weights": normal_values(streams_of[2], (LAYERS, EXPERTS, ROWS, FF), 0.5, 4.0, ((1, 2), (2, 16)), jnp.float32),
        "shadow": normal_values(streams_of[3], (LAYERS, EXPERTS, ROWS, FF), 0.5, 4.0, ((1, 2), (2, 16)), jnp.float32),
        "counts": draw_counts(jax.random.fold_in(streams_of[5], 71), 0),
    }


step_size = 0.5
clip_level = 1.0

def reference(activations, out_grads, weights, shadow, counts):
    totals = lax.optimization_barrier(jnp.sum(counts, axis=1, dtype=jnp.int32))
    all_weights = []
    all_shadow = []
    for layer_index in range(LAYERS):
        loads = totals[layer_index].astype(jnp.float32)
        mean_load = jnp.mean(loads)

        def update_one(item):
            inputs, cotangent, current, smooth, own_load = item
            summed = jnp.dot(inputs.T, cotangent, preferred_element_type=jnp.float32)
            numel = summed.shape[0] * summed.shape[1]
            root_mean = jnp.sqrt(jnp.sum(summed * summed) / numel)
            factor = step_size * (own_load / mean_load) * clip_level / jnp.maximum(root_mean, clip_level)
            updated = current - factor * summed
            beta = own_load / (own_load + mean_load)
            return (updated, smooth + beta * (updated - smooth))
        updated, smoothed = lax.map(update_one, (activations[layer_index], out_grads[layer_index], weights[layer_index], shadow[layer_index], loads))
        all_weights.append(updated)
        all_shadow.append(smoothed)
    return (jnp.stack(all_weights), jnp.stack(all_shadow))
```

```python
import jax
import jax.numpy as jnp
from jax import lax
from jax.sharding import PartitionSpec as P


GROUP = ("dp", "shard")
CHUNKS = 4
step_size = 0.5
clip_level = 1.0


def bits_of(size):
    return [1 << k for k in range(size.bit_length() - 1)]


def swap(value, size, bit):
    return lax.ppermute(value, GROUP, [(g, g ^ bit) for g in range(size)])


def summed_over(value, axis):
    size = lax.axis_size(axis)
    total = value
    for bit in bits_of(size):
        total = total + lax.ppermute(total, axis, [(g, g ^ bit) for g in range(size)])
    return total


def relative_rows(inputs, order, own_rows, me):
    rows = inputs.shape[1]
    position = lax.broadcasted_iota(jnp.int32, (rows, rows), 0)
    block = position // own_rows
    relative = jnp.zeros_like(block)
    for place, bit in enumerate(reversed(order)):
        relative = relative + ((block >> place) & 1) * bit
    source = (relative ^ me) * own_rows + position % own_rows
    pick = (source == lax.broadcasted_iota(jnp.int32, (rows, rows), 1)).astype(inputs.dtype)
    return lax.dot_general(
        pick, inputs, (((1,), (1,)), ((), ())), preferred_element_type=jnp.float32
    ).astype(inputs.dtype)


def issue_order(jobs, links, own_rows, size):
    now, done, free, arrival, stage = 0.0, [], {}, [0.0] * len(jobs), [0] * len(jobs)
    while len(done) < sum(len(order) + 1 for order, _ in jobs):
        open_jobs = [j for j in range(len(jobs)) if stage[j] <= len(jobs[j][0])]
        begun = [j for j in open_jobs if stage[j] > 0 and arrival[j] <= now]
        fresh = [j for j in open_jobs if stage[j] == 0]
        if begun:
            job = min(begun, key=lambda j: arrival[j])
        elif fresh:
            job = fresh[0]
        else:
            job = min(open_jobs, key=lambda j: arrival[j])
            now = arrival[job]
        order, width = jobs[job]
        at = stage[job]
        now += 2.5
        if at < len(order):
            link = links[order[at]]
            rate = 6e5 if link == "core" else 5e4
            sent = (size >> (at + 1)) * own_rows * width * 4 / rate
            free[link] = max(free.get(link, 0.0), now) + sent
            arrival[job] = free[link] + 2.0
        done.append((job, at))
        stage[job] += 1
    return done


def reduce_all(jobs, links, lefts, rights, own_rows, size):
    arrived = [[] for _ in jobs]
    results = [None] * len(jobs)
    waiting = None

    def settle(job, at, value):
        order = jobs[job][0]
        if at < len(order):
            arrived[job].append(swap(value, size, order[at]))
        else:
            results[job] = value

    for job, at in issue_order(jobs, links, own_rows, size):
        left = lefts[job]
        if waiting is not None:
            before, step, value = waiting
            left, value = lax.optimization_barrier((left, value))
            settle(before, step, value)
        low = 0 if at == len(jobs[job][0]) else (size >> (at + 1)) * own_rows
        high = (size >> at) * own_rows
        value = lax.dot_general(
            left[low:high],
            rights[job],
            (((1,), (0,)), ((), ())),
            preferred_element_type=jnp.float32,
        )
        for got in arrived[job]:
            value = value + got[low:high]
        waiting = (job, at, value)
    settle(*waiting)
    return results


def exchange_order(dp, shard):
    shard_bits = bits_of(shard)
    dp_bits = [bit * shard for bit in bits_of(dp)]
    first, rest = shard_bits[:1], shard_bits[1:]
    links = {bit: "dp" for bit in dp_bits} | {bit: "shard" for bit in rest}
    links |= {bit: "core" for bit in first}
    plain = first + rest + dp_bits
    early = first + dp_bits[:1] + rest + dp_bits[1:]
    return links, plain, early


def all_jobs(layers, columns, plain, early):
    width = columns // CHUNKS
    return [(early if chunk == 1 else plain, width) for _ in range(layers) for chunk in range(CHUNKS)]


def on_device(activations, out_grads, weights, shadow, counts):
    layers, _, _, columns = out_grads.shape
    experts = counts.shape[-1]
    own_rows = weights.shape[2]
    size = lax.axis_size(GROUP)
    me = lax.axis_index(GROUP)
    links, plain, early = exchange_order(lax.axis_size("dp"), lax.axis_size("shard"))
    jobs = all_jobs(layers, columns, plain, early)
    own_slot = (jnp.arange(experts) == lax.axis_index("expert")).astype(jnp.float32)
    load_sums = summed_over(counts[:, 0, :].astype(jnp.float32), "expert")

    width = columns // CHUNKS
    lefts, rights = [], []
    for layer in range(layers):
        inputs = activations[layer, 0]
        rows_of = {}
        for order in (plain, early):
            rows_of[tuple(order)] = relative_rows(inputs, order, own_rows, me)
        for chunk in range(CHUNKS):
            order = early if chunk == 1 else plain
            lefts.append(rows_of[tuple(order)])
            rights.append(out_grads[layer, 0, :, chunk * width : (chunk + 1) * width])
    pieces = reduce_all(jobs, links, lefts, rights, own_rows, size)
    grads = [pieces[layer * CHUNKS : (layer + 1) * CHUNKS] for layer in range(layers)]
    squares = jnp.stack([sum(jnp.sum(piece * piece) for piece in layer) for layer in grads])
    totals = jnp.concatenate([load_sums.reshape(-1), squares])
    for axis in ("shard", "dp"):
        totals = summed_over(totals, axis)
    load_totals = totals[: layers * experts].reshape(layers, experts)
    total_squares = totals[layers * experts :]

    all_weights, all_shadow = [], []
    for layer in range(layers):
        loads = load_totals[layer]
        own_load = jnp.sum(loads * own_slot)
        mean_load = jnp.mean(loads)
        root_mean = jnp.sqrt(total_squares[layer] / (own_rows * size * columns))
        factor = (
            step_size * (own_load / mean_load) * clip_level / jnp.maximum(root_mean, clip_level)
        )
        beta = own_load / (own_load + mean_load)
        summed = jnp.concatenate(grads[layer], axis=1)
        updated = weights[layer, 0] - factor * summed
        previous = shadow[layer, 0]
        all_weights.append(updated)
        all_shadow.append(previous + beta * (updated - previous))
    return (jnp.stack(all_weights)[:, None], jnp.stack(all_shadow)[:, None])


def solution(mesh):
    split = P(None, "expert", ("dp", "shard"), None)
    in_specs = (split, split, split, split, P(None, ("dp", "expert", "shard"), None))

    def step(activations, out_grads, weights, shadow, counts):
        return jax.shard_map(
            on_device, mesh=mesh, in_specs=in_specs, out_specs=(split, split), check_vma=False
        )(activations, out_grads, weights, shadow, counts)

    return step
```

```python
import jax
import jax.numpy as jnp
from jax import lax
from jax.sharding import PartitionSpec as P


GROUP = ("dp", "shard")
FIRST, LATER = (16, 28, 28, 24, 16), (24, 16, 24, 28, 20)
EARLY = (1,)
step_size = 0.5
clip_level = 1.0


def bits_of(size):
    return [1 << k for k in range(size.bit_length() - 1)]


def swap(value, size, bit):
    return lax.ppermute(value, GROUP, [(g, g ^ bit) for g in range(size)])


def summed_over(value, axis):
    size = lax.axis_size(axis)
    total = value
    for bit in bits_of(size):
        total = total + lax.ppermute(total, axis, [(g, g ^ bit) for g in range(size)])
    return total


def relative_rows(inputs, order, own_rows, me):
    rows = inputs.shape[1]
    position = lax.broadcasted_iota(jnp.int32, (rows, rows), 0)
    block = position // own_rows
    relative = jnp.zeros_like(block)
    for place, bit in enumerate(reversed(order)):
        relative = relative + ((block >> place) & 1) * bit
    source = (relative ^ me) * own_rows + position % own_rows
    pick = (source == lax.broadcasted_iota(jnp.int32, (rows, rows), 1)).astype(inputs.dtype)
    return lax.dot_general(
        pick, inputs, (((1,), (1,)), ((), ())), preferred_element_type=jnp.float32
    ).astype(inputs.dtype)


def issue_order(jobs, links, own_rows, size):
    now, done, free, arrival, stage = 0.0, [], {}, [0.0] * len(jobs), [0] * len(jobs)
    while len(done) < sum(len(order) + 1 for order, _ in jobs):
        open_jobs = [j for j in range(len(jobs)) if stage[j] <= len(jobs[j][0])]
        begun = [j for j in open_jobs if stage[j] > 0 and arrival[j] <= now]
        fresh = [j for j in open_jobs if stage[j] == 0]
        if begun:
            job = min(begun, key=lambda j: arrival[j])
        elif fresh:
            job = fresh[0]
        else:
            job = min(open_jobs, key=lambda j: arrival[j])
            now = arrival[job]
        order, width = jobs[job]
        at = stage[job]
        now += 3.6 if at == len(order) else 2.7 if at else 2.2
        if at < len(order):
            link = links[order[at]]
            far = link == "dp" and at == len(order) - 1
            rate = 6e5 if link == "core" else 2.6e4 if far else 5.15e4
            sent = (size >> (at + 1)) * own_rows * width * 4 / rate
            free[link] = max(free.get(link, 0.0), now) + sent
            arrival[job] = free[link] + 2.0
        done.append((job, at))
        stage[job] += 1
    return done


def reduce_all(jobs, links, lefts, rights, own_rows, size):
    arrived = [[] for _ in jobs]
    results = [None] * len(jobs)
    waiting = None

    def settle(job, at, value):
        order = jobs[job][0]
        if at < len(order):
            arrived[job].append(swap(value, size, order[at]))
        else:
            results[job] = value

    for job, at in issue_order(jobs, links, own_rows, size):
        left = lefts[job]
        if waiting is not None:
            before, step, value = waiting
            left, value = lax.optimization_barrier((left, value))
            settle(before, step, value)
        low = 0 if at == len(jobs[job][0]) else (size >> (at + 1)) * own_rows
        high = (size >> at) * own_rows
        value = lax.dot_general(
            left[low:high],
            rights[job],
            (((1,), (0,)), ((), ())),
            preferred_element_type=jnp.float32,
        )
        for got in arrived[job]:
            value = value + got[low:high]
        waiting = (job, at, value)
    settle(*waiting)
    return results


def exchange_order(dp, shard):
    shard_bits = bits_of(shard)
    dp_bits = [bit * shard for bit in bits_of(dp)]
    first, rest = shard_bits[:1], shard_bits[1:]
    links = {bit: "dp" for bit in dp_bits} | {bit: "shard" for bit in rest}
    links |= {bit: "core" for bit in first}
    plain = first + rest + dp_bits
    early = first + dp_bits[:1] + rest + dp_bits[1:]
    return links, plain, early


def all_jobs(layers, columns, plain, early):
    jobs = []
    for layer in range(layers):
        shares = FIRST if layer == 0 else LATER
        unit = columns // sum(shares)
        for chunk, share in enumerate(shares):
            is_early = layer == 0 and chunk in EARLY
            jobs.append((layer, unit * sum(shares[:chunk]), early if is_early else plain, unit * share))
    return jobs


def on_device(activations, out_grads, weights, shadow, counts):
    layers, _, _, columns = out_grads.shape
    experts = counts.shape[-1]
    own_rows = weights.shape[2]
    size = lax.axis_size(GROUP)
    me = lax.axis_index(GROUP)
    links, plain, early = exchange_order(lax.axis_size("dp"), lax.axis_size("shard"))
    plan = all_jobs(layers, columns, plain, early)
    jobs = [job[2:] for job in plan]
    own_slot = (jnp.arange(experts) == lax.axis_index("expert")).astype(jnp.float32)
    load_sums = summed_over(counts[:, 0, :].astype(jnp.float32), "expert")

    lefts, rights = [], []
    rows_of = {}
    for layer, begin, order, width in plan:
        key = (layer, tuple(order))
        if key not in rows_of:
            rows_of[key] = relative_rows(activations[layer, 0], order, own_rows, me)
        lefts.append(rows_of[key])
        rights.append(out_grads[layer, 0, :, begin : begin + width])
    pieces = reduce_all(jobs, links, lefts, rights, own_rows, size)
    grads = [[p for p, job in zip(pieces, plan) if job[0] == layer] for layer in range(layers)]
    squares = jnp.stack([sum(jnp.sum(piece * piece) for piece in layer) for layer in grads])
    totals = jnp.concatenate([load_sums.reshape(-1), squares])
    for axis in ("shard", "dp"):
        totals = summed_over(totals, axis)
    load_totals = totals[: layers * experts].reshape(layers, experts)
    total_squares = totals[layers * experts :]

    own_load = jnp.sum(load_totals * own_slot, axis=1)
    mean_load = jnp.mean(load_totals, axis=1)
    root_mean = jnp.sqrt(total_squares / (own_rows * size * columns))
    factors = step_size * (own_load / mean_load) * clip_level / jnp.maximum(root_mean, clip_level)
    betas = own_load / (own_load + mean_load)
    all_weights, all_shadow = [], []
    for layer in range(layers):
        factor, beta = factors[layer], betas[layer]
        summed = jnp.concatenate(grads[layer], axis=1)
        updated = weights[layer, 0] - factor * summed
        previous = shadow[layer, 0]
        all_weights.append(updated)
        all_shadow.append(previous + beta * (updated - previous))
    return (jnp.stack(all_weights)[:, None], jnp.stack(all_shadow)[:, None])


def solution(mesh):
    split = P(None, "expert", ("dp", "shard"), None)
    in_specs = (split, split, split, split, P(None, ("dp", "expert", "shard"), None))

    def step(activations, out_grads, weights, shadow, counts):
        return jax.shard_map(
            on_device, mesh=mesh, in_specs=in_specs, out_specs=(split, split), check_vma=False
        )(activations, out_grads, weights, shadow, counts)

    return step
```
